32 devices in a mesh: dp: 2 (over y), expert: 16 (over z, x, core).
Axes of the slice: x: 2, y: 2, z: 4, core: 2. Of those that a mesh axis runs over, the one named last changes fastest.
Arguments:
- routed: bfloat16 [4096, 7168], P(('dp', 'expert')), may hold values from -160 to 160
- expert_ids: int32 [4096, 8], P(('dp', 'expert')), may hold values from 0 to 127, all different within a row
- norm_gain: bfloat16 [7168], replicated, may hold values from 0.099609375 to 1.8984375
- gate_weight: bfloat16 [16, 7168, 2048], P('expert', None, 'dp'), may hold values from -0.0625 to 0.0625
- up_weight: bfloat16 [16, 7168, 2048], P('expert', None, 'dp'), may hold values from -0.0625 to 0.0625
- down_weight: bfloat16 [16, 2048, 7168], P('expert', 'dp'), may hold values from -0.125 to 0.125
- old_place: int32 [16], replicated, may hold values from 0 to 127, as said below
- new_place: int32 [16], replicated, may hold values from 0 to 127, as said below
- probe_ids: int32 [1280], P(('dp', 'expert')), may hold values from 0 to 127
Outputs:
- expert_load: float32 [128], P('expert')
- expert_energy: float32 [128], P('expert')
- probe_out: bfloat16 [1280, 7168], P(('dp', 'expert'))
The draws below stay inside these ranges and needn't reach their ends.
Inputs may be any that keep to these rules, and one draw needn't show every extreme that they name: `old_place`: 16 different experts. `new_place`: the same 16 experts as old_place, in some order.
All inputs are finite; a program needn't handle non-finite values.
Results may differ from the reference program's by a relative error of at most 0.012.
Values may be sent and summed in bfloat16 or wider, within the bound.
No kernel may reach another device: no remote copies, remote signals or barrier semaphores. Data moves between devices by JAX's collectives and lax.ppermute only.
A program may use at most 128 MiB of HBM per device.

```python
import jax
import jax.numpy as jnp
from jax import lax

D = 7168
FF = 2048
TOP = 8
TOK_DEV = 128
PROBE = 40
EXPERTS = 128
SLOTS = 16
TOKENS = 4096
PROBES = 1280
N_DP = 2


def draw_routed(key, part):
    first = jax.random.fold_in(key, 101)
    second = jax.random.fold_in(key, 202)
    third = jax.random.fold_in(key, 303)
    row_scale = jnp.exp(jax.random.uniform(second, (TOKENS, 1), minval=-1.15, maxval=1.15))
    column_scale = jnp.exp(jax.random.uniform(third, (1, D), minval=-1.15, maxval=1.15))
    rising = jnp.exp(jnp.log(3.0) * (jnp.arange(TOKENS, dtype=jnp.float32) / TOKENS - 0.5))[:, None]
    values = jnp.clip(jax.random.normal(first, (TOKENS, D)), -4.0, 4.0)
    return (values * row_scale * column_scale * rising).astype(jnp.bfloat16)


def draw_plan(key):
    base = jax.random.fold_in(key, 17)
    chosen = jax.random.permutation(jax.random.fold_in(base, 1), EXPERTS)[:SLOTS]
    order = jax.random.permutation(jax.random.fold_in(base, 2), SLOTS)
    return (chosen.astype(jnp.int32), jnp.take(chosen, order).astype(jnp.int32))


def draw_old_place(key, part):
    return draw_plan(key)[0]


def draw_new_place(key, part):
    return draw_plan(key)[1]


def with_ends(values, own_key, least, high):
    longest = values.shape.index(max(values.shape))
    spots = []
    for shift in (0, 1):
        where = [jax.random.randint(jax.random.fold_in(own_key, axis), (), 0, length) for axis, length in enumerate(values.shape)]
        where[longest] = (where[longest] + shift) % values.shape[longest]
        spots.append(tuple(where))
    return values.at[spots[0]].set(least).at[spots[1]].set(high)


def block_levels(stream_key, extent, pieces, low, top_value):
    level, own = 1.0, jax.random.fold_in(stream_key, 6)
    for dim, parts in pieces:
        steps = jnp.exp(jax.random.uniform(jax.random.fold_in(own, dim), (parts,), jnp.float32, low / len(pieces), top_value / len(pieces)))
        level = level * jnp.repeat(steps, extent[dim] // parts).reshape([-1 if axis == dim else 1 for axis in range(len(extent))])
    return level


def picks_of(rng, rows, count, top, lift):
    ranking = jax.random.permutation(jax.random.fold_in(rng, 1), count)
    pull = ranking
    for power in range(3):
        pull = pull * pull // count
    pull = pull * lift // count
    tickets = jax.random.randint(jax.random.fold_in(rng, 2), (rows, count), 0, 4096) + pull
    holders = jax.random.permutation(jax.random.fold_in(rng, 3), rows)[jnp.arange(count) % rows]
    tickets = jnp.where(jnp.arange(rows)[:, None] == holders[None, :], 1 << 14, tickets)
    merit = tickets * count + jnp.arange(count)
    return lax.top_k(merit.astype(jnp.int32), top)[1].astype(jnp.int32)


def noise(stream_key, shape, deviation, most, cuts=(), kind=jnp.bfloat16):
    array = deviation * jax.random.normal(stream_key, shape, jnp.float32)
    if cuts:
        array = array * block_levels(stream_key, shape, cuts, -0.22, 0.18)
    return jnp.clip(array, -most, most).astype(kind)


def setup_inputs(seed: int = 0) -> dict:
    seeds = jax.random.split(jax.random.key(seed), 10)
    return {
        "routed": draw_routed(jax.random.fold_in(seeds[9], 71), 0),
        "expert_ids": picks_of(seeds[1], TOKENS, EXPERTS, TOP, 1024),
        "norm_gain": jnp.clip(1.0 + 0.18 * jax.random.normal(seeds[2], (D,), jnp.float32), 0.099609375, 1.8984375).astype(jnp.bfloat16),
        "gate_weight": noise(seeds[3], (SLOTS, D, FF), D ** -0.5, 0.0625, ((0, 16), (2, 2))),
        "up_weight": noise(seeds[4], (SLOTS, D, FF), D ** -0.5, 0.0625, ((0, 16), (2, 2))),
        "down_weight": noise(seeds[5], (SLOTS, FF, D), FF ** -0.5, 0.125, ((0, 16), (1, 2))),
        "old_place": draw_old_place(jax.random.fold_in(seeds[9], 71), 0),
        "new_place": draw_new_place(jax.random.fold_in(seeds[9], 71), 0),
        "probe_ids": with_ends(jax.random.randint(seeds[8], (PROBES,), 0, TOK_DEV), jax.random.fold_in(seeds[8], 1), 0, TOK_DEV - 1).astype(jnp.int32),
    }


epsilon = 1e-06

def block_stats(block):
    token_rows, id_block = block
    features = token_rows.astype(jnp.float32)
    mean_square = lax.optimization_barrier(jnp.sum(features * features, axis=1)) / D
    positions = jnp.arange(EXPERTS, dtype=jnp.int32)
    onehot = lax.optimization_barrier(jnp.sum((id_block[:, :, None] == positions[None, None, :]).astype(jnp.float32), axis=1))
    columns = jnp.stack([jnp.ones_like(mean_square), mean_square])
    return (jnp.dot(columns, onehot, precision=lax.Precision.HIGHEST), mean_square)

def reference(routed, expert_ids, norm_gain, gate_weight, up_weight, down_weight, old_place, new_place, probe_ids):
    blocks = TOKENS // TOK_DEV
    stats, mean_square = lax.map(block_stats, (routed.reshape(blocks, TOK_DEV, D), expert_ids.reshape(blocks, TOK_DEV, TOP)))
    totals = lax.optimization_barrier(jnp.sum(stats, axis=0))
    counts = totals[0]
    expert_load = counts * EXPERTS / (TOKENS * TOP)
    expert_energy = totals[1] / counts
    mean_square = mean_square.reshape(TOKENS)
    offsets = jnp.arange(PROBES, dtype=jnp.int32) // PROBE * TOK_DEV
    picked = (offsets + probe_ids).astype(jnp.int32)
    picked_rows = jnp.take(routed, picked, axis=0).astype(jnp.float32)
    scale = lax.rsqrt(jnp.take(mean_square, picked) + epsilon)
    normed = (picked_rows * scale[:, None] * norm_gain.astype(jnp.float32)[None, :]).astype(jnp.bfloat16)
    grouped = normed.reshape(N_DP, SLOTS, PROBE, D)
    slot_index = jnp.arange(SLOTS, dtype=jnp.int32)
    hidden_block = FF // N_DP

    def per_slot(slot_number):
        holder = jnp.sum(jnp.where(old_place == new_place[slot_number], slot_index, 0)).astype(jnp.int32)
        inputs = lax.dynamic_index_in_dim(grouped, slot_number, 1, keepdims=False).reshape(N_DP * PROBE, D)
        gate_matrix = lax.dynamic_index_in_dim(gate_weight, holder, 0, keepdims=False)
        up_matrix = lax.dynamic_index_in_dim(up_weight, holder, 0, keepdims=False)
        down_matrix = lax.dynamic_index_in_dim(down_weight, holder, 0, keepdims=False)
        gate_value = jnp.dot(inputs, gate_matrix, preferred_element_type=jnp.float32)
        up_value = jnp.dot(inputs, up_matrix, preferred_element_type=jnp.float32)
        hidden = (jax.nn.silu(gate_value) * up_value).astype(jnp.bfloat16)
        running = jnp.zeros((N_DP * PROBE, D), jnp.float32)
        for group_index in range(N_DP):
            lower = group_index * hidden_block
            partial_value = jnp.dot(hidden[:, lower:lower + hidden_block], down_matrix[lower:lower + hidden_block], preferred_element_type=jnp.float32).astype(jnp.bfloat16)
            partial_value = lax.optimization_barrier(partial_value)
            running = running + partial_value.astype(jnp.float32)
        return running.astype(jnp.bfloat16).reshape(N_DP, PROBE, D)
    results = lax.map(per_slot, slot_index)
    probe_out = jnp.transpose(results, (1, 0, 2, 3)).reshape(PROBES, D)
    return (expert_load, expert_energy, probe_out)
```

```python
import functools
import math

import jax
import jax.numpy as jnp
from jax import lax
from jax.experimental import pallas as pl
from jax.experimental.pallas import tpu as pltpu
from jax.sharding import PartitionSpec as P

EXP_DEV = 8
TOP = 8
LANES = 128
epsilon = 1e-06
VMEM = pltpu.MemorySpace.VMEM
SMEM = pltpu.MemorySpace.SMEM


def prepare_body(z_ref, probe_ref, routed_ref, ids_ref, gain_ref, stats_ref, *rest):
    pieces, raw_ref = rest[:-1], rest[-1]
    tokens, width = routed_ref.shape
    probes = probe_ref.shape[0]
    experts = stats_ref.shape[1]
    step = 512
    rows = lax.broadcasted_iota(jnp.int32, (probes, tokens), 0)
    lanes = lax.broadcasted_iota(jnp.int32, (probes, tokens), 1)
    wanted = jnp.zeros((probes, tokens), jnp.int32)
    for p in range(probes):
        wanted = jnp.where(rows == p, probe_ref[p], wanted)
    pick = (wanted == lanes).astype(jnp.float32).astype(jnp.bfloat16)

    def gather(k, carry):
        total, chosen = carry
        columns = pl.ds(pl.multiple_of(k * step, step), step)
        block = routed_ref[:, columns]
        values = block.astype(jnp.float32)
        taken = jnp.dot(pick, block, preferred_element_type=jnp.float32)
        raw_ref[:, columns] = taken.astype(jnp.bfloat16)
        for c in range(step // LANES):
            part = values[:, c * LANES : (c + 1) * LANES]
            total = total + part * part
            part = taken[:, c * LANES : (c + 1) * LANES]
            chosen = chosen + part * part
        return total, chosen

    total, chosen = lax.fori_loop(
        0,
        width // step,
        gather,
        (jnp.zeros((tokens, LANES), jnp.float32), jnp.zeros((probes, LANES), jnp.float32)),
    )
    scale = lax.rsqrt(jnp.sum(chosen, axis=1, keepdims=True) / width + epsilon)
    part = width // len(pieces)
    for s, piece in enumerate(pieces):
        start = (z_ref[0] ^ s) * part
        columns = pl.ds(pl.multiple_of(start, LANES), part)
        values = raw_ref[:, columns].astype(jnp.float32)
        gain = gain_ref[:, columns].astype(jnp.float32)
        piece[...] = (values * scale * gain).astype(jnp.bfloat16)
    mean_square = jnp.sum(total.T, axis=0, keepdims=True) / width
    which = lax.broadcasted_iota(jnp.int32, (experts, tokens), 0)
    member = jnp.zeros((experts, tokens), jnp.float32)
    for k in range(ids_ref.shape[0]):
        member = member + (ids_ref[k : k + 1, :] == which).astype(jnp.float32)
    row = lax.broadcasted_iota(jnp.int32, (8, tokens), 0)
    columns = jnp.where(row == 0, 1.0, jnp.broadcast_to(mean_square, (8, tokens)))
    stats_ref[...] = lax.dot_general(
        columns,
        member,
        (((1,), (1,)), ((), ())),
        precision=lax.Precision.HIGHEST,
        preferred_element_type=jnp.float32,
    )


def prepare(z, probe_ids, routed, ids, gain, experts, parts):
    width = routed.shape[1]
    probes = probe_ids.shape[0]
    piece = jax.ShapeDtypeStruct((probes, width // parts), jnp.bfloat16)
    spec = pl.BlockSpec(memory_space=VMEM)
    out = pl.pallas_call(
        prepare_body,
        out_shape=(jax.ShapeDtypeStruct((8, experts), jnp.float32),) + (piece,) * parts,
        in_specs=[pl.BlockSpec(memory_space=SMEM)] * 2 + [spec] * 3,
        out_specs=(spec,) * (parts + 1),
        scratch_shapes=[pltpu.VMEM((probes, width), jnp.bfloat16)],
        cost_estimate=pl.CostEstimate(
            flops=8 * routed.size, bytes_accessed=4 * routed.size, transcendentals=0
        ),
        name="prepare",
    )(z, probe_ids, routed, ids, gain[None])
    return out[0], out[1:]


def gate_up_kernel(groups, *refs):
    xs, refs = refs[:groups], refs[groups:]
    gate_w, up_w, hidden_ref, gate_acc, up_acc = refs
    step = pl.program_id(0)

    @pl.when(step == 0)
    def _():
        gate_acc[...] = jnp.zeros_like(gate_acc)
        up_acc[...] = jnp.zeros_like(up_acc)

    x = jnp.concatenate([x_ref[...] for x_ref in xs], axis=0)
    gate_acc[...] += jnp.dot(x, gate_w[...], preferred_element_type=jnp.float32)
    up_acc[...] += jnp.dot(x, up_w[...], preferred_element_type=jnp.float32)

    @pl.when(step == pl.num_programs(0) - 1)
    def _():
        hidden_ref[...] = (jax.nn.silu(gate_acc[...]) * up_acc[...]).astype(jnp.bfloat16)


def gate_up(xs, gate_w, up_w, block=896):
    rows = sum(x.shape[0] for x in xs)
    width, units = gate_w.shape
    return pl.pallas_call(
        functools.partial(gate_up_kernel, len(xs)),
        grid=(width // block,),
        out_shape=jax.ShapeDtypeStruct((rows, units), jnp.bfloat16),
        in_specs=[pl.BlockSpec((x.shape[0], block), lambda i: (0, i)) for x in xs]
        + [pl.BlockSpec((block, units), lambda i: (i, 0))] * 2,
        out_specs=pl.BlockSpec((rows, units), lambda i: (0, 0)),
        scratch_shapes=[pltpu.VMEM((rows, units), jnp.float32)] * 2,
        cost_estimate=pl.CostEstimate(
            flops=4 * rows * width * units, bytes_accessed=4 * width * units, transcendentals=0
        ),
        name="gate_up",
    )(*xs, gate_w, up_w)


def down_kernel(groups, hidden_ref, down_w, *outs):
    product = jnp.dot(hidden_ref[...], down_w[...], preferred_element_type=jnp.float32)
    rows = product.shape[0] // groups
    for g, out in enumerate(outs):
        out[...] = product[g * rows : (g + 1) * rows].astype(jnp.bfloat16)


def down(hidden, down_w, groups, block=896):
    units, width = down_w.shape
    rows = hidden.shape[0] // groups
    return pl.pallas_call(
        functools.partial(down_kernel, groups),
        grid=(width // block,),
        out_shape=(jax.ShapeDtypeStruct((rows, width), jnp.bfloat16),) * groups,
        in_specs=[
            pl.BlockSpec(hidden.shape, lambda i: (0, 0)),
            pl.BlockSpec((units, block), lambda i: (0, i)),
        ],
        out_specs=(pl.BlockSpec((rows, block), lambda i: (0, i)),) * groups,
        cost_estimate=pl.CostEstimate(
            flops=2 * rows * groups * width * units,
            bytes_accessed=2 * width * units,
            transcendentals=0,
        ),
        name="down",
    )(hidden, down_w)


def swap(value, axis, size, bits):
    return lax.ppermute(value, axis, [(i, i ^ bits) for i in range(size)])


def flatten_blocks(array, slots):
    length = array.size // slots
    lanes = math.gcd(length, 128)
    return array.reshape(slots, length // lanes, lanes)


def relay_rows(array, sources):
    shaped = flatten_blocks(array, sources.shape[0])
    spread = lax.all_to_all(shaped, "expert", split_axis=0, concat_axis=0, tiled=True)
    chosen = jnp.take(spread, sources, axis=0, mode="clip")
    moved = lax.all_to_all(chosen, "expert", split_axis=0, concat_axis=0, tiled=True)
    return moved.reshape(array.shape)


def total_stats(stats, slots, dps):
    bit = 1
    while bit < dps:
        stats = stats + swap(stats, "dp", dps, bit)
        bit *= 2
    bit = 1
    while bit < slots:
        stats = stats + swap(stats, "expert", slots, bit)
        bit *= 2
    return stats


def on_device(
    routed,
    expert_ids,
    norm_gain,
    gate_weight,
    up_weight,
    down_weight,
    old_place,
    new_place,
    probe_ids,
):
    slots = lax.axis_size("expert")
    dps = lax.axis_size("dp")
    experts = EXP_DEV * slots
    tokens = routed.shape[0] * dps * slots
    me = lax.axis_index("expert")
    stats, pieces = prepare(
        jnp.zeros((1,), jnp.int32), probe_ids, routed, expert_ids.T, norm_gain, experts, 1
    )
    slot_index = jnp.arange(slots, dtype=jnp.int32)
    matches = new_place[:, None] == old_place[None, :]
    sources = jnp.sum(jnp.where(matches, slot_index[None, :], 0), axis=1)
    targets = jnp.sum(jnp.where(matches, slot_index[:, None], 0), axis=0)
    arrived = relay_rows(pieces[0], targets)
    rows = [arrived] + [swap(arrived, "dp", dps, s) for s in range(1, dps)]
    hidden = gate_up(rows, gate_weight[0], up_weight[0])
    partial = down(hidden, down_weight[0], dps)
    running = partial[0].astype(jnp.float32)
    for s in range(1, dps):
        running = running + swap(partial[s], "dp", dps, s).astype(jnp.float32)
    probe_out = relay_rows(running.astype(jnp.bfloat16), sources)
    totals = total_stats(stats, slots, dps)
    owned = lax.dynamic_slice_in_dim(totals, me * EXP_DEV, EXP_DEV, 1)
    expert_load = owned[0] * experts / (tokens * TOP)
    expert_energy = owned[1] / owned[0]
    return (expert_load, expert_energy, probe_out)


def solution(mesh):
    in_specs = (
        P(("dp", "expert"), None),
        P(("dp", "expert"), None),
        P(),
        P("expert", None, "dp"),
        P("expert", None, "dp"),
        P("expert", "dp", None),
        P(),
        P(),
        P(("dp", "expert")),
    )
    out_specs = (P("expert"), P("expert"), P(("dp", "expert"), None))
    return jax.shard_map(
        on_device, mesh=mesh, in_specs=in_specs, out_specs=out_specs, check_vma=False
    )
```

```python
import functools
import math

import jax
import jax.numpy as jnp
from jax import lax
from jax.experimental import pallas as pl
from jax.experimental.pallas import tpu as pltpu
from jax.sharding import PartitionSpec as P

EXP_DEV = 8
TOP = 8
LANES = 128
epsilon = 1e-06
VMEM = pltpu.MemorySpace.VMEM
SMEM = pltpu.MemorySpace.SMEM
HBM = pltpu.MemorySpace.HBM


def prepare_body(
    me_ref, probe_hbm, old_hbm, new_hbm, routed_hbm, ids_hbm, gain_hbm, stats_ref, picks_ref, *rest
):
    pieces, rest = rest[:-9], rest[-9:]
    probe_ref, old_ref, new_ref, routed_ref, ids_ref, gain_ref, raw_ref, small_sems, sems = rest
    tokens, width = routed_ref.shape
    probes = probe_ref.shape[0]
    experts = stats_ref.shape[1]
    slots = old_ref.shape[0]
    parts = len(pieces)
    stride = slots // parts
    part = width // parts
    me = me_ref[0]
    small = [
        pltpu.make_async_copy(source, target, small_sems.at[k])
        for k, (source, target) in enumerate(
            (
                (probe_hbm, probe_ref),
                (old_hbm, old_ref),
                (new_hbm, new_ref),
                (ids_hbm, ids_ref),
                (gain_hbm, gain_ref),
            )
        )
    ]
    large = [
        pltpu.make_async_copy(
            routed_hbm.at[:, pl.ds(q * part, part)],
            routed_ref.at[:, pl.ds(q * part, part)],
            sems.at[q],
        )
        for q in range(parts)
    ]
    small[0].start()
    for copy in large:
        copy.start()
    for copy in small[1:]:
        copy.start()
    rows = lax.broadcasted_iota(jnp.int32, (probes, tokens), 0)
    lanes = lax.broadcasted_iota(jnp.int32, (probes, tokens), 1)
    wanted = jnp.zeros((probes, tokens), jnp.int32)
    small[0].wait()
    for p in range(probes):
        wanted = jnp.where(rows == p, probe_ref[p], wanted)
    pick = (wanted == lanes).astype(jnp.float32).astype(jnp.bfloat16)
    total = jnp.zeros((tokens, LANES), jnp.float32)
    chosen = jnp.zeros((probes, LANES), jnp.float32)
    for q in range(parts):
        large[q].wait()
        columns = slice(q * part, (q + 1) * part)
        taken = jnp.dot(pick, routed_ref[:, columns], preferred_element_type=jnp.float32)
        raw_ref[:, columns] = taken.astype(jnp.bfloat16)
        for c in range(part // LANES):
            start = q * part + c * LANES
            piece = routed_ref[:, start : start + LANES].astype(jnp.float32)
            total = total + piece * piece
        for c in range(part // LANES):
            piece = taken[:, c * LANES : (c + 1) * LANES]
            chosen = chosen + piece * piece
    scale = lax.rsqrt(jnp.sum(chosen, axis=1, keepdims=True) / width + epsilon)
    for copy in small[1:]:
        copy.wait()
    for s, piece in enumerate(pieces):
        start = ((me // stride) ^ s) * part
        columns = pl.ds(pl.multiple_of(start, LANES), part)
        values = raw_ref[:, columns].astype(jnp.float32)
        gain = gain_ref[columns].astype(jnp.float32)[None, :]
        piece[...] = (values * scale * gain).astype(jnp.bfloat16)
    mean_square = jnp.sum(total.T, axis=0, keepdims=True) / width
    which = lax.broadcasted_iota(jnp.int32, (experts, tokens), 0)
    member = jnp.zeros((experts, tokens), jnp.float32)
    for k in range(ids_ref.shape[0]):
        member = member + (ids_ref[k : k + 1, :] == which).astype(jnp.float32)
    row = lax.broadcasted_iota(jnp.int32, (8, tokens), 0)
    columns = jnp.where(row == 0, 1.0, jnp.broadcast_to(mean_square, (8, tokens)))
    stats_ref[...] = lax.dot_general(
        columns,
        member,
        (((1,), (1,)), ((), ())),
        precision=lax.Precision.HIGHEST,
        preferred_element_type=jnp.float32,
    )
    for t in range(parts):
        for direction, (keys, seek) in enumerate(((old_ref, new_ref), (new_ref, old_ref))):
            key = keys[me ^ (t * stride)]
            found = jnp.int32(0)
            for j in range(slots):
                found = jnp.where(seek[j] == key, jnp.int32(j), found)
            picks_ref[direction * parts + t] = found ^ me


def prepare(me, probe_ids, old_place, new_place, routed, ids, gain, experts, parts):
    tokens, width = routed.shape
    probes = probe_ids.shape[0]
    slots = old_place.shape[0]
    piece = jax.ShapeDtypeStruct((probes, width // parts), jnp.bfloat16)
    vmem, smem = pl.BlockSpec(memory_space=VMEM), pl.BlockSpec(memory_space=SMEM)
    out = pl.pallas_call(
        prepare_body,
        out_shape=(
            jax.ShapeDtypeStruct((8, experts), jnp.float32),
            jax.ShapeDtypeStruct((2 * parts,), jnp.int32),
        )
        + (piece,) * parts,
        in_specs=[smem] + [pl.BlockSpec(memory_space=HBM)] * 6,
        out_specs=(vmem, smem) + (vmem,) * parts,
        scratch_shapes=[
            pltpu.SMEM((probes,), jnp.int32),
            pltpu.SMEM((slots,), jnp.int32),
            pltpu.SMEM((slots,), jnp.int32),
            pltpu.VMEM((tokens, width), jnp.bfloat16),
            pltpu.VMEM(ids.shape, jnp.int32),
            pltpu.VMEM((width,), jnp.bfloat16),
            pltpu.VMEM((probes, width), jnp.bfloat16),
            pltpu.SemaphoreType.DMA((5,)),
            pltpu.SemaphoreType.DMA((parts,)),
        ],
        compiler_params=limit(routed, *([piece] * 3 * parts)),
        cost_estimate=pl.CostEstimate(
            flops=8 * routed.size, bytes_accessed=4 * routed.size, transcendentals=0
        ),
        name="prepare",
    )(me, *[fixed(a) for a in (probe_ids, old_place, new_place, routed, ids, gain)])
    return out[0], out[1], out[2:]


def fixed(array):
    return pltpu.with_memory_space_constraint(array, HBM)


def limit(*arrays):
    return pltpu.CompilerParams(vmem_limit_bytes=4 * 1024 * 1024 + sum(2 * a.size * a.dtype.itemsize for a in arrays))


def gate_up_kernel(groups, shift, first, final, cuts, z_ref, *refs):
    xs, refs = refs[:groups], refs[groups:]
    weights, refs = refs[:2], refs[2:]
    if not first:
        sums_in, refs = refs[:2], refs[2:]
    outs, (gate_buf, up_buf, sems) = refs[:-3], refs[-3:]
    part = xs[0].shape[1]
    cut = part // cuts
    start = (z_ref[0] ^ shift) * part
    copies = []
    for k in range(cuts):
        for m, (weight, buf) in enumerate(zip(weights, (gate_buf, up_buf))):
            rows = pl.ds(pl.multiple_of(start + k * cut, LANES), cut)
            copy = pltpu.make_async_copy(weight.at[rows], buf.at[pl.ds(k * cut, cut)], sems.at[m, k])
            copy.start()
            copies.append(copy)
    x = jnp.concatenate([x_ref[...] for x_ref in xs], axis=0)
    sums = [0.0, 0.0] if first else [ref[...] for ref in sums_in]
    for k in range(cuts):
        for m, buf in enumerate((gate_buf, up_buf)):
            copies[2 * k + m].wait()
            sums[m] = sums[m] + jnp.dot(
                x[:, k * cut : (k + 1) * cut],
                buf[k * cut : (k + 1) * cut, :],
                preferred_element_type=jnp.float32,
            )
    if final:
        outs[0][...] = (jax.nn.silu(sums[0]) * sums[1]).astype(jnp.bfloat16)
    else:
        outs[0][...] = sums[0]
        outs[1][...] = sums[1]


def gate_up(z, shift, pieces, gate_w, up_w, sums, final, cuts=4):
    groups = len(pieces)
    one_rows, part = pieces[0].shape
    rows = groups * one_rows
    units = gate_w.shape[1]
    if part % (cuts * LANES):
        cuts = 2
    vmem, smem = pl.BlockSpec(memory_space=VMEM), pl.BlockSpec(memory_space=SMEM)
    hbm = pl.BlockSpec(memory_space=HBM)
    acc = jax.ShapeDtypeStruct((rows, units), jnp.float32)
    extra = () if sums is None else sums
    buf = pltpu.VMEM((part, units), jnp.bfloat16)
    return pl.pallas_call(
        functools.partial(gate_up_kernel, groups, shift, sums is None, final, cuts),
        in_specs=[smem] + [vmem] * groups + [hbm] * 2 + [vmem] * len(extra),
        out_specs=vmem if final else (vmem, vmem),
        out_shape=jax.ShapeDtypeStruct((rows, units), jnp.bfloat16) if final else (acc, acc),
        scratch_shapes=[buf, buf, pltpu.SemaphoreType.DMA((2, cuts))],
        compiler_params=limit(*pieces, acc, acc, acc, acc, jax.ShapeDtypeStruct((part, units), jnp.bfloat16)),
        cost_estimate=pl.CostEstimate(
            flops=4 * rows * part * units,
            bytes_accessed=4 * part * units,
            transcendentals=0,
        ),
        name="gate_up",
    )(z, *pieces, fixed(gate_w), fixed(up_w), *extra)


def down_kernel(groups, shift, cuts, z_ref, hidden_ref, down_w, *refs):
    outs, (buf, sems) = refs[:-2], refs[-2:]
    rows, part = outs[0].shape
    cut = part // cuts
    start = (z_ref[0] ^ shift) * part
    copies = []
    for k in range(cuts):
        columns = pl.ds(pl.multiple_of(start + k * cut, LANES), cut)
        copy = pltpu.make_async_copy(down_w.at[:, columns], buf.at[k], sems.at[k])
        copy.start()
        copies.append(copy)
    hidden = hidden_ref[...]
    for k in range(cuts):
        copies[k].wait()
        product = jnp.dot(hidden, buf[k], preferred_element_type=jnp.float32).astype(jnp.bfloat16)
        for g, out in enumerate(outs):
            out[:, k * cut : (k + 1) * cut] = product[g * rows : (g + 1) * rows]


def down(z, shift, hidden, down_w, groups, parts, cuts=2):
    units, width = down_w.shape
    rows = hidden.shape[0] // groups
    part = width // parts
    vmem, smem = pl.BlockSpec(memory_space=VMEM), pl.BlockSpec(memory_space=SMEM)
    out = jax.ShapeDtypeStruct((rows, part), jnp.bfloat16)
    return pl.pallas_call(
        functools.partial(down_kernel, groups, shift, cuts),
        in_specs=[smem, vmem, pl.BlockSpec(memory_space=HBM)],
        out_specs=(vmem,) * groups,
        out_shape=(out,) * groups,
        scratch_shapes=[
            pltpu.VMEM((cuts, units, part // cuts), jnp.bfloat16),
            pltpu.SemaphoreType.DMA((cuts,)),
        ],
        compiler_params=limit(hidden, *([out] * 2 * groups), jax.ShapeDtypeStruct((part, units), jnp.bfloat16)),
        cost_estimate=pl.CostEstimate(
            flops=2 * rows * groups * part * units,
            bytes_accessed=2 * part * units,
            transcendentals=0,
        ),
        name="down",
    )(z, hidden, fixed(down_w))


def choose_kernel(direction, picks_ref, *refs):
    parts = picks_ref.shape[0] // 2
    held, outs = refs[:-parts], refs[-parts:]
    for t, out in enumerate(outs):
        picked = picks_ref[direction * parts + t]
        for k in range(len(held)):

            @pl.when(picked == k)
            def _():
                out[...] = held[k][...]


def choose(direction, picks, held):
    parts = picks.shape[0] // 2
    piece = jax.ShapeDtypeStruct(held[0].shape, held[0].dtype)
    vmem, smem = pl.BlockSpec(memory_space=VMEM), pl.BlockSpec(memory_space=SMEM)
    return pl.pallas_call(
        functools.partial(choose_kernel, direction),
        out_shape=(piece,) * parts,
        in_specs=[smem] + [vmem] * len(held),
        out_specs=(vmem,) * parts,
        compiler_params=limit(*held, *([piece] * parts)),
        cost_estimate=pl.CostEstimate(
            flops=held[0].size * len(held), bytes_accessed=4 * held[0].size * parts, transcendentals=0
        ),
        name="choose",
    )(picks, *held)


def join_kernel(z_ref, *refs):
    pieces, out = refs[:-1], refs[-1]
    part = pieces[0].shape[1]
    for s, piece in enumerate(pieces):
        start = (z_ref[0] ^ s) * part
        out[:, pl.ds(pl.multiple_of(start, LANES), part)] = piece[...]


def join(z, pieces):
    rows, part = pieces[0].shape
    vmem, smem = pl.BlockSpec(memory_space=VMEM), pl.BlockSpec(memory_space=SMEM)
    return pl.pallas_call(
        join_kernel,
        out_shape=jax.ShapeDtypeStruct((rows, part * len(pieces)), pieces[0].dtype),
        in_specs=[smem] + [vmem] * len(pieces),
        out_specs=vmem,
        compiler_params=limit(*pieces, *pieces),
        name="join",
    )(z, *pieces)


def swap(value, axis, size, bits):
    return lax.ppermute(value, axis, [(i, i ^ bits) for i in range(size)])


def tie(value, *others):
    return lax.optimization_barrier((value, *others))[0]


def relay(direction, picks, pieces, slots, riders=()):
    riders = list(riders)
    parts = len(pieces)
    stride = slots // parts
    held = [None] * slots
    moved = [swap(pieces[s], "expert", slots, s * stride) if s else pieces[0] for s in range(parts)]
    before = []
    for s in range(parts):
        here = tie(moved[s], *before)
        if s and riders:
            here = riders.pop(0)(here)
        before = []
        if s:
            base = (s - 1) * stride
            for x in range(2, stride, 2):
                held[base + x + 1] = swap(held[base + x], "expert", slots, 1)
                before.append(held[base + x + 1])
        base = s * stride
        held[base] = here
        for x in range(2, stride, 2):
            held[base + x] = swap(here, "expert", slots, x)
        held[base + 1] = swap(here, "expert", slots, 1)
        before.append(held[base + 1])
    base = (parts - 1) * stride
    for x in range(2, stride, 2):
        held[base + x + 1] = swap(held[base + x], "expert", slots, 1)
    chosen = choose(direction, picks, held)
    return [swap(chosen[s], "expert", slots, s * stride) if s else chosen[0] for s in range(parts)]


class Totals:
    def __init__(self, stats, hops):
        self.stats, self.hops = stats, list(hops)

    def hop(self, axis, size, bit, other):
        self.stats = self.stats + swap(self.stats, axis, size, bit)
        self.stats, other = lax.optimization_barrier((self.stats, other))
        return other

    def riders(self):
        return [functools.partial(self.hop, *hop) for hop in self.hops]


def on_device(
    routed,
    expert_ids,
    norm_gain,
    gate_weight,
    up_weight,
    down_weight,
    old_place,
    new_place,
    probe_ids,
):
    slots = lax.axis_size("expert")
    dps = lax.axis_size("dp")
    experts = EXP_DEV * slots
    tokens = routed.shape[0] * dps * slots
    me = lax.axis_index("expert")
    parts = math.gcd(slots // 2, 4)
    stride = slots // parts
    mine = me[None].astype(jnp.int32)
    z = mine // stride
    stats, picks, pieces = prepare(
        mine, probe_ids, old_place, new_place, routed, expert_ids.T, norm_gain, experts, parts
    )
    bits = lambda size: [1 << k for k in range(size.bit_length() - 1)]
    hops = [("dp", dps, bit) for bit in bits(dps)] + [("expert", slots, bit) for bit in bits(slots)]
    stats = Totals(stats, hops)
    riders = stats.riders()
    pieces = relay(0, picks, pieces, slots, riders[:-2])
    riders = riders[-2:]
    sums = None
    history = []
    for s in range(parts):
        final = s == parts - 1
        piece = pieces[s]
        if s > 1:
            piece = tie(piece, *history[s - 2])
        if s and riders:
            piece = riders.pop(0)(piece)
        group = [piece] + [swap(piece, "dp", dps, g) for g in range(1, dps)]
        sums = gate_up(z, s, group, gate_weight[0], up_weight[0], sums, final)
        history.append(sums)
    totals = stats.stats
    result = [None] * parts
    hidden = sums
    order = [*range(1, parts), 0]
    for k, s in enumerate(order):
        if k > 1:
            hidden = tie(hidden, result[order[k - 2]])
        partial = down(z, s, hidden, down_weight[0], dps, parts)
        running = partial[0].astype(jnp.float32)
        for g in range(1, dps):
            running = running + swap(partial[g], "dp", dps, g).astype(jnp.float32)
        result[s] = running.astype(jnp.bfloat16)
    probe_out = join(z, relay(1, picks, result, slots))
    owned = lax.dynamic_slice_in_dim(totals, me * EXP_DEV, EXP_DEV, 1)
    expert_load = owned[0] * experts / (tokens * TOP)
    expert_energy = owned[1] / owned[0]
    return (expert_load, expert_energy, probe_out)


def solution(mesh):
    in_specs = (
        P(("dp", "expert"), None),
        P(("dp", "expert"), None),
        P(),
        P("expert", None, "dp"),
        P("expert", None, "dp"),
        P("expert", "dp", None),
        P(),
        P(),
        P(("dp", "expert")),
    )
    out_specs = (P("expert"), P("expert"), P(("dp", "expert"), None))
    return jax.shard_map(
        on_device, mesh=mesh, in_specs=in_specs, out_specs=out_specs, check_vma=False
    )
```
